32 devices in a mesh: grp: 4 (over y, x), blk: 8 (over z, core).
Axes of the slice: x: 2, y: 2, z: 4, core: 2. Of those that a mesh axis runs over, the one named last changes fastest.
Arguments:
- embeddings: bfloat16 [8192, 1024], P(('grp', 'blk')), may hold values from -40 to 40
- cluster_ids: int32 [8192], P(('grp', 'blk')), may hold values from 0 to 3, as said below
Outputs:
- dup_score: float32 [8192], P(('grp', 'blk'))
The draws below stay inside these ranges and needn't reach their ends.
Inputs may be any that keep to these rules, and one draw needn't show every extreme that they name: `cluster_ids`: cluster c belongs to owner group c. Among the rows of one device at most 128 belong to any one cluster; in every draw there is an owner group each of whose clusters has exactly 128 rows on every device.
All inputs are finite; a program needn't handle non-finite values.
Results may differ from the reference program's by a relative error of at most 0.00041.
Values may be sent and summed in bfloat16 or wider, within the bound.
No kernel may reach another device: no remote copies, remote signals or barrier semaphores. Data moves between devices by JAX's collectives and lax.ppermute only.
A program may use at most 64 MiB of HBM per device.

```python
import jax
import jax.numpy as jnp
from jax import lax

D = 1024
ROWS_DEV = 256
CLUS_GRP = 1
CLUSTERS = 4
CAPC = 128
DOCS = 8192
N_GRP = 4
N_BLK = 8


def joint_ids(key):
    base_key = jax.random.fold_in(key, 11)
    device_count = N_GRP * N_BLK
    slot_total = 2 * ROWS_DEV
    per_cluster = slot_total // CLUSTERS
    favour_key, order_key = jax.random.split(base_key, 2)
    favoured = jax.random.randint(favour_key, (), 0, N_GRP)
    slot_cluster = jnp.arange(slot_total, dtype=jnp.int32) // per_cluster
    slot_owner = slot_cluster // CLUS_GRP

    def one_device(device_key):
        pick_key, shuffle_key = jax.random.split(device_key)
        shuffled = jax.random.permutation(pick_key, slot_total)
        priority = shuffled + jnp.where(slot_owner == favoured, 0, slot_total)
        chosen = slot_cluster[jnp.argsort(priority)[:ROWS_DEV]]
        return jax.random.permutation(shuffle_key, chosen)
    labels = jax.vmap(one_device)(jax.random.split(order_key, device_count))
    return labels.reshape(-1).astype(jnp.int32)


def draw_cluster_ids(key, part):
    return joint_ids(key)


def draw_embeddings(key, part):
    labels = joint_ids(key)
    base_key = jax.random.fold_in(key, 23)
    sub_keys = jax.random.split(base_key, 7)
    family_count = max(DOCS // (CLUSTERS * 8), 2)
    family = jnp.minimum(jax.random.randint(sub_keys[0], (DOCS,), 0, family_count), jax.random.randint(sub_keys[1], (DOCS,), 0, family_count))
    family_row = labels * family_count + family
    family_weight = jnp.exp(jax.random.uniform(sub_keys[2], (DOCS, 1), jnp.float32, jnp.log(0.6), jnp.log(1.2)))
    noise_weight = jax.random.uniform(sub_keys[3], (DOCS, 1), jnp.float32, 0.3, 0.6)
    centers = jax.random.normal(sub_keys[4], (CLUSTERS, D), jnp.float32)
    families = jax.random.normal(sub_keys[5], (CLUSTERS * family_count, D), jnp.float32)
    noise_part = jax.random.normal(sub_keys[6], (DOCS, D), jnp.float32)
    mixture = 0.5 * centers[labels] + family_weight * families[family_row] + noise_weight * noise_part
    return jnp.clip(mixture, -40.0, 40.0).astype(jnp.bfloat16)


def setup_inputs(seed: int = 0) -> dict:
    arg_keys = jax.random.split(jax.random.key(seed), 3)
    return {
        "embeddings": draw_embeddings(jax.random.fold_in(arg_keys[2], 71), 0),
        "cluster_ids": draw_cluster_ids(jax.random.fold_in(arg_keys[2], 71), 0),
    }


def reference(embeddings, cluster_ids):
    widened = embeddings.astype(jnp.float32)
    squared = lax.optimization_barrier(jnp.sum(widened * widened, axis=1, keepdims=True)) + 1e-06
    inverse_norm = lax.rsqrt(squared)
    unit_rows = (widened * inverse_norm).astype(jnp.bfloat16)
    ordering = jnp.argsort(cluster_ids, stable=True).astype(jnp.int32)
    cluster_sizes = jnp.zeros((CLUSTERS,), jnp.int32).at[cluster_ids].add(jnp.ones((DOCS,), jnp.int32))
    starts = (jnp.cumsum(cluster_sizes) - cluster_sizes).astype(jnp.int32)
    largest = N_GRP * N_BLK * CAPC
    padded = jnp.concatenate([ordering, jnp.zeros((largest,), jnp.int32)])

    def one_cluster(cluster_index):
        picked = lax.dynamic_slice_in_dim(padded, starts[cluster_index], largest).astype(jnp.int32)
        positions = jnp.arange(largest, dtype=jnp.int32)
        alive_mask = positions < cluster_sizes[cluster_index]
        chosen_rows = unit_rows[picked]
        similar = jnp.dot(chosen_rows, chosen_rows.T, preferred_element_type=jnp.float32)
        weights = jax.nn.sigmoid(20.0 * (similar - 0.7))
        keep_mask = alive_mask[:, None] & alive_mask[None, :] & (positions[:, None] != positions[None, :])
        row_sums = lax.optimization_barrier(jnp.sum(jnp.where(keep_mask, weights, jnp.zeros_like(weights)), axis=1))
        return (jnp.where(alive_mask, row_sums, jnp.zeros_like(row_sums)), picked)
    sums_all, picked_all = lax.map(one_cluster, jnp.arange(CLUSTERS, dtype=jnp.int32))
    soft = jnp.zeros((DOCS,), jnp.float32).at[picked_all.reshape(-1)].add(sums_all.reshape(-1))
    return jnp.log1p(soft)
```

```python
import functools

import jax
import jax.numpy as jnp
from jax import lax
from jax.experimental import pallas as pl
from jax.experimental.pallas import tpu as pltpu
from jax.sharding import PartitionSpec as P


THRESHOLD = 0.7
SHARPNESS = 20.0
TAG_ROWS = 8


def pack_kernel(rows_ref, ids_ref, out_ref):
    rows, width = rows_ref.shape
    wide = rows_ref[...].astype(jnp.float32)
    squared = jnp.sum(wide * wide, axis=1, keepdims=True) + 1e-06
    out_ref[:rows, :] = (wide * lax.rsqrt(squared)).astype(jnp.bfloat16)
    tags = jnp.broadcast_to(ids_ref[...].astype(jnp.float32) + 1.0, (TAG_ROWS, rows))
    out_ref[rows:, :rows] = tags.astype(jnp.bfloat16)
    out_ref[rows:, rows:] = jnp.zeros((TAG_ROWS, width - rows), jnp.bfloat16)


def pack(rows, ids):
    count, width = rows.shape
    return pl.pallas_call(
        pack_kernel,
        out_shape=jax.ShapeDtypeStruct((count + TAG_ROWS, width), jnp.bfloat16),
        name="pack",
    )(rows, ids.reshape(1, count))


def tiles(left_blocks, right_blocks, plan, state):
    rows = left_blocks[0].shape[0] - TAG_ROWS
    slots = []
    for per_left in plan:
        for _, slot, col_slot, _ in per_left:
            for name in (slot, col_slot):
                if name is not None and name not in slots:
                    slots.append(name)
    known = [slot for slot in slots if slot in state]

    def body(*refs):
        given = len(left_blocks) + len(right_blocks)
        old = dict(zip(known, refs[given : given + len(known)]))
        out_refs = dict(zip(slots, refs[given + len(known) :]))
        left_refs, right_refs = refs[: len(left_blocks)], refs[len(left_blocks) : given]
        sums = {slot: old[slot][...] for slot in known}

        def gain(slot, value):
            sums[slot] = sums[slot] + value if slot in sums else value

        half = rows // 2
        for left_ref, per_left in zip(left_refs, plan):
            tags = left_ref[rows:, :rows].astype(jnp.float32)
            left_tags = jnp.transpose(tags)[:, :1]
            across = {}
            for right, slot, col_slot, drop_self in per_left:
                right_ref = right_refs[right]
                similar = lax.dot_general(
                    left_ref[:rows, :],
                    right_ref[:rows, :],
                    (((1,), (1,)), ((), ())),
                    preferred_element_type=jnp.float32,
                )
                weights = 1.0 / (1.0 + jnp.exp(SHARPNESS * THRESHOLD - SHARPNESS * similar))
                right_tags = right_ref[rows : rows + 1, :rows].astype(jnp.float32)
                keep = left_tags == right_tags
                if drop_self:
                    down = lax.broadcasted_iota(jnp.int32, (rows, rows), 0)
                    along = lax.broadcasted_iota(jnp.int32, (rows, rows), 1)
                    keep = keep & (down != along)
                weights = jnp.where(keep, weights, 0.0)
                folded = weights[:, :half] + weights[:, half:]
                across[slot] = across[slot] + folded if slot in across else folded
                if col_slot is not None:
                    gain(col_slot, jnp.sum(weights, axis=0, keepdims=True))
            for slot, value in across.items():
                gain(slot, jnp.sum(jnp.transpose(value), axis=0, keepdims=True))
        for slot in slots:
            out_refs[slot][...] = sums[slot]

    results = pl.pallas_call(
        body,
        out_shape=[jax.ShapeDtypeStruct((1, rows), jnp.float32) for _ in slots],
        name="tiles",
    )(*left_blocks, *right_blocks, *[state[slot] for slot in known])
    return {**state, **dict(zip(slots, results))}


def shards(embeddings, cluster_ids, groups, members):
    chips = members // 2
    far = chips // 2

    def partner(block):
        return lax.ppermute(block, "blk", [(i, i ^ 1) for i in range(members)])

    def across_plane(block, mask):
        return lax.ppermute(block, "grp", [(i, i ^ mask) for i in range(groups)])

    def routes(step):
        pairs = []
        for chip in range(chips):
            ahead = (chip + step) % chips
            if 2 * step == chips:
                if chip >= far:
                    continue
                pair = (chip, ahead) if chip % 2 == 0 else (ahead, chip)
            else:
                pair = (chip, ahead)
            pairs.append(pair)
        return pairs

    def visit(block, step, back=False):
        pairs = [(b, a) if back else (a, b) for a, b in routes(step)]
        return lax.ppermute(
            block, "blk", [(2 * a + c, 2 * b + c) for a, b in pairs for c in range(2)]
        )

    own = pack(embeddings, cluster_ids)
    masks = range(1, groups)
    steps = range(1, far + 1)
    visitors = {steps[0]: visit(own, steps[0])}
    plane = {mask: across_plane(own, mask) for mask in masks}
    for step in steps[1:]:
        visitors[step] = visit(own, step)
    plane[0] = own
    other = partner(own)

    state = {}
    near = [mask for mask in range(groups) if mask.bit_count() < 2]
    rest = [mask for mask in range(groups) if mask.bit_count() >= 2]

    def add(state, lefts, masks):
        plan = []
        for name, _ in lefts:
            per_left = []
            for right, mask in enumerate(masks):
                col_slot = ("col", mask) if name[1] else None
                per_left.append((right, name, col_slot, name == ("own", 0) and mask == 0))
            plan.append(per_left)
        return tiles([block for _, block in lefts], [plane[mask] for mask in masks], plan, state)

    homes = [(("own", 0), own), (("other", 0), other)]
    state = add(state, homes, [0])
    state = add(state, homes, near[1:])
    first = steps[0]
    guests = [(("own", first), visitors[first]), (("other", first), partner(visitors[first]))]
    state = add(state, guests, near)
    state = add(state, homes + guests, rest)
    for step in steps[1:]:
        arrived = visitors[step]
        state = add(state, [(("own", step), arrived)], near + rest)
        state = add(state, [(("other", step), partner(arrived))], near + rest)

    total = state[("own", 0)] + state[("col", 0)]
    crossed = partner(jnp.concatenate([state[("other", step)] for step in (0, *steps)], axis=0))
    total = total + crossed[:1]
    for mask in masks:
        total = total + across_plane(state[("col", mask)], mask)
    for step in steps:
        total = total + visit(state[("own", step)] + crossed[step : step + 1], step, back=True)
    return jnp.log1p(total.reshape(-1))


def solution(mesh):
    body = functools.partial(shards, groups=mesh.shape["grp"], members=mesh.shape["blk"])
    return jax.shard_map(
        body,
        mesh=mesh,
        in_specs=(P(("grp", "blk"), None), P(("grp", "blk"))),
        out_specs=P(("grp", "blk")),
        check_vma=False,
    )
```

```python
import functools

import jax
import jax.numpy as jnp
from jax import lax
from jax.experimental import pallas as pl
from jax.experimental.pallas import tpu as pltpu
from jax.sharding import PartitionSpec as P


THRESHOLD = 0.7
SHARPNESS = 20.0
TAG_ROWS = 8
KERNEL_BYTES = 8 * 1024 * 1024


def near(block):
    return pltpu.with_memory_space_constraint(block, pltpu.VMEM)


def pack_kernel(rows_ref, ids_ref, out_ref):
    rows, width = rows_ref.shape
    wide = rows_ref[...].astype(jnp.float32)
    squared = jnp.sum(wide * wide, axis=1, keepdims=True) + 1e-06
    out_ref[:rows, :] = (wide * lax.rsqrt(squared)).astype(jnp.bfloat16)
    tags = jnp.broadcast_to(ids_ref[...].astype(jnp.float32) + 1.0, (TAG_ROWS, rows))
    out_ref[rows:, :rows] = tags.astype(jnp.bfloat16)
    out_ref[rows:, rows:] = jnp.zeros((TAG_ROWS, width - rows), jnp.bfloat16)


def pack(rows, ids):
    count, width = rows.shape
    return pl.pallas_call(
        pack_kernel,
        out_shape=pltpu.VMEM((count + TAG_ROWS, width), jnp.bfloat16),
        compiler_params=pltpu.CompilerParams(vmem_limit_bytes=KERNEL_BYTES),
        name="pack",
    )(rows, ids.reshape(1, count))


def tiles(left_blocks, right_blocks, plan, state):
    rows = left_blocks[0].shape[0] - TAG_ROWS
    slots = []
    for per_left in plan:
        for _, slot, col_slot, _ in per_left:
            for name in (slot, col_slot):
                if name is not None and name not in slots:
                    slots.append(name)
    known = [slot for slot in slots if slot in state]

    def body(*refs):
        given = len(left_blocks) + len(right_blocks)
        old = dict(zip(known, refs[given : given + len(known)]))
        out_refs = dict(zip(slots, refs[given + len(known) :]))
        left_refs, right_refs = refs[: len(left_blocks)], refs[len(left_blocks) : given]
        sums = {slot: old[slot][...] for slot in known}

        def gain(slot, value):
            sums[slot] = sums[slot] + value if slot in sums else value

        half = rows // 2
        for left_ref, per_left in zip(left_refs, plan):
            tags = left_ref[rows:, :rows].astype(jnp.float32)
            left_tags = jnp.transpose(tags)[:, :1]
            across = {}
            for right, slot, col_slot, drop_self in per_left:
                right_ref = right_refs[right]
                similar = lax.dot_general(
                    left_ref[:rows, :],
                    right_ref[:rows, :],
                    (((1,), (1,)), ((), ())),
                    preferred_element_type=jnp.float32,
                )
                weights = 1.0 / (1.0 + jnp.exp(SHARPNESS * THRESHOLD - SHARPNESS * similar))
                right_tags = right_ref[rows : rows + 1, :rows].astype(jnp.float32)
                keep = left_tags == right_tags
                if drop_self:
                    down = lax.broadcasted_iota(jnp.int32, (rows, rows), 0)
                    along = lax.broadcasted_iota(jnp.int32, (rows, rows), 1)
                    keep = keep & (down != along)
                weights = jnp.where(keep, weights, 0.0)
                folded = weights[:, :half] + weights[:, half:]
                across[slot] = across[slot] + folded if slot in across else folded
                if col_slot is not None:
                    gain(col_slot, jnp.sum(weights, axis=0, keepdims=True))
            for slot, value in across.items():
                gain(slot, jnp.sum(jnp.transpose(value), axis=0, keepdims=True))
        for slot in slots:
            out_refs[slot][...] = sums[slot]

    results = pl.pallas_call(
        body,
        out_shape=[pltpu.VMEM((1, rows), jnp.float32) for _ in slots],
        compiler_params=pltpu.CompilerParams(vmem_limit_bytes=KERNEL_BYTES),
        name="tiles",
    )(*map(near, [*left_blocks, *right_blocks, *[state[slot] for slot in known]]))
    return {**state, **dict(zip(slots, results))}


def shards(embeddings, cluster_ids, groups, members):
    chips = members // 2
    far = chips // 2

    def partner(block):
        return lax.ppermute(block, "blk", [(i, i ^ 1) for i in range(members)])

    def across_plane(block, mask):
        return lax.ppermute(block, "grp", [(i, i ^ mask) for i in range(groups)])

    def routes(step):
        pairs = []
        for chip in range(chips):
            ahead = (chip + step) % chips
            if 2 * step == chips:
                if chip >= far:
                    continue
                pair = (chip, ahead) if chip % 2 == 0 else (ahead, chip)
            else:
                pair = (chip, ahead)
            pairs.append(pair)
        return pairs

    def visit(block, step, back=False):
        pairs = [(b, a) if back else (a, b) for a, b in routes(step)]
        return lax.ppermute(
            block, "blk", [(2 * a + c, 2 * b + c) for a, b in pairs for c in range(2)]
        )

    own = pack(embeddings, cluster_ids)
    masks = range(1, groups)
    steps = range(1, far + 1)
    visitors = {steps[0]: visit(own, steps[0])}
    plane = {mask: across_plane(own, mask) for mask in masks}
    for step in steps[1:]:
        visitors[step] = visit(own, step)
    plane[0] = own
    other = partner(own)

    state = {}
    close = [mask for mask in range(groups) if mask.bit_count() < 2]
    rest = [mask for mask in range(groups) if mask.bit_count() >= 2]

    def add(state, lefts, masks):
        plan = []
        for name, _ in lefts:
            per_left = []
            for right, mask in enumerate(masks):
                col_slot = ("col", mask) if name[1] else None
                per_left.append((right, name, col_slot, name == ("own", 0) and mask == 0))
            plan.append(per_left)
        return tiles([block for _, block in lefts], [plane[mask] for mask in masks], plan, state)

    homes = [(("own", 0), own), (("other", 0), other)]
    state = add(state, homes, [0])
    state = add(state, homes, close[1:])
    first = steps[0]
    guests = [(("own", first), visitors[first]), (("other", first), partner(visitors[first]))]
    state = add(state, guests, close)
    state = add(state, homes + guests, rest)
    for step in steps[1:]:
        arrived = visitors[step]
        state = add(state, [(("own", step), arrived)], close + rest)
        state = add(state, [(("other", step), partner(arrived))], close + rest)

    total = state[("own", 0)] + state[("col", 0)]
    crossed = partner(jnp.concatenate([state[("other", step)] for step in (0, *steps)], axis=0))
    total = total + crossed[:1]
    for mask in masks:
        total = total + across_plane(state[("col", mask)], mask)
    for step in steps:
        total = total + visit(state[("own", step)] + crossed[step : step + 1], step, back=True)
    return jnp.log1p(total.reshape(-1))


def solution(mesh):
    body = functools.partial(shards, groups=mesh.shape["grp"], members=mesh.shape["blk"])
    return jax.shard_map(
        body,
        mesh=mesh,
        in_specs=(P(("grp", "blk"), None), P(("grp", "blk"))),
        out_specs=P(("grp", "blk")),
        check_vma=False,
    )
```
